128 devices in a mesh: gx: 4 (over y), gy: 4 (over x_hi, core), gz: 8 (over z, x_lo).
Axes of the slice: x: 4 (x_hi: 2, x_lo: 2; x = x_hi * 2 + x_lo), y: 4, z: 4, core: 2. Of those that a mesh axis runs over, the one named last changes fastest.
Arguments:
- concentration: float32 [512, 512, 512], P('gz', 'gx', 'gy'), may hold values from -1 to 1
Outputs:
- concentration_next: float32 [512, 512, 512], P('gz', 'gx', 'gy')
The draws below stay inside these ranges and needn't reach their ends.
All inputs are finite; a program needn't handle non-finite values.
Results may differ from the reference program's by a relative error of at most 0.00011.
Values sent between devices are 32-bit elements; how exact they have to be, the bound alone decides.
A program may use at most 192 MiB of HBM per device.

```python
import jax
import jax.numpy as jnp
from jax import lax

NX = 512
NY = 512
NZ = 512


def draw_concentration(key, part):
    key_sign = jax.random.fold_in(key, 11)
    key_size = jax.random.fold_in(key, 12)
    x_position = jnp.arange(NX, dtype=jnp.float32) / (NX - 1)
    sign_field = jnp.where(jax.random.bernoulli(key_sign, 0.5, (NZ, NX, NY)), 1.0, -1.0)
    magnitude = jax.random.uniform(key_size, (NZ, NX, NY), jnp.float32, 0.85, 1.0)
    amplitude = 0.2 + 0.8 * x_position
    result = amplitude[None, :, None] * sign_field * magnitude
    return result.astype(jnp.float32)


def setup_inputs(seed: int = 0) -> dict:
    keys = jax.random.split(jax.random.key(seed), 2)
    concentration = draw_concentration(jax.random.fold_in(keys[1], 71), 0)
    return dict(concentration=concentration)


step_length = 0.2
stiffness = 0.25

def hartley_table(length):
    indices = jnp.arange(length, dtype=jnp.int32)
    product = indices[:, None] * indices[None, :] % length
    angles = 2.0 * jnp.pi / length * product.astype(jnp.float32)
    return ((jnp.cos(angles) + jnp.sin(angles)) / jnp.sqrt(float(length))).astype(jnp.float32)

def wave_square(length):
    indices = jnp.arange(length, dtype=jnp.int32)
    folded = jnp.minimum(indices, length - indices).astype(jnp.float32)
    wave = 2.0 * jnp.pi / length * folded
    return wave * wave

def along_axis(matrix, source, axis_number):
    highest = lax.Precision.HIGHEST
    if axis_number == 0:
        return jnp.einsum('ij,jxy->ixy', matrix, source, precision=highest)
    if axis_number == 1:
        return jnp.einsum('ij,zjy->ziy', matrix, source, precision=highest)
    return jnp.einsum('ij,zxj->zxi', matrix, source, precision=highest)

def transform(spectral, source):
    out_field = along_axis(spectral[0], source, 0)
    out_field = along_axis(spectral[1], out_field, 1)
    return along_axis(spectral[2], out_field, 2)

def reference(concentration):
    potential = concentration * concentration * concentration - concentration
    mobility = 1.05 - concentration * concentration
    mean_mobility = jnp.sum(mobility) / (NX * NY * NZ)
    divergence = jnp.zeros_like(concentration)
    for axis_number in range(3):
        next_potential = jnp.roll(potential, -1, axis=axis_number)
        next_mobility = jnp.roll(mobility, -1, axis=axis_number)
        flux = 0.5 * (mobility + next_mobility) * (next_potential - potential)
        divergence = divergence + (flux - jnp.roll(flux, 1, axis=axis_number))
    update = concentration + step_length * divergence
    spectral = (hartley_table(NZ), hartley_table(NX), hartley_table(NY))
    spectrum = transform(spectral, update)
    wave_sum = wave_square(NZ)[:, None, None] + wave_square(NX)[None, :, None] + wave_square(NY)[None, None, :]
    spectrum = spectrum / (1.0 + step_length * stiffness * mean_mobility * wave_sum * wave_sum)
    return transform(spectral, spectrum)
```

```python
import functools

import jax
import jax.numpy as jnp
import numpy as np
from jax import lax
from jax.experimental import pallas as pl
from jax.experimental.pallas import tpu as pltpu
from jax.sharding import PartitionSpec as P

MESH = pl.DeviceIdType.MESH
F32, BF16 = jnp.float32, jnp.bfloat16

step_length = 0.2
stiffness = 0.25

N = 512
HALF = N // 2
BZ, BX, BY = 64, 128, 128
CHUNK = 16
Z_OFFSETS = ((1, 0), (0, 1), (3, 0), (2, 0), (1, 1), (3, 1), (2, 1))


def split_table(matrix):
    high = matrix.astype(np.float32).astype(jnp.bfloat16)
    low = (matrix - high.astype(np.float64)).astype(np.float32).astype(jnp.bfloat16)
    return high, low


def tables():
    index = np.arange(N)
    angle = 2.0 * np.pi / N * (index[:, None] * index[None, :] % N)
    hartley = (np.cos(angle) + np.sin(angle)) / np.sqrt(N)
    even, odd = hartley[0::2, :HALF], hartley[1::2, :HALF]
    left, right = [], []
    for matrix in (even, odd, odd.T):
        high, low = split_table(matrix)
        left.append(np.concatenate([high, low, high], axis=1))
    for matrix in (even, odd.T, odd):
        high, low = split_table(matrix)
        right.append(np.concatenate([high, low, high], axis=0))
    return np.stack(left), np.stack(right)


def thirds(a, axis):
    high = a.astype(BF16)
    low = (a - high.astype(F32)).astype(BF16)
    return jnp.concatenate([high, high, low], axis=axis)


def matmul(a, b):
    return jnp.dot(a, b, preferred_element_type=F32)


def wave_of(position):
    true = jnp.where(position < HALF, 2 * position, 2 * position - (N - 1))
    folded = jnp.minimum(true, N - true).astype(F32)
    wave = (2.0 * np.pi / N) * folded
    return wave * wave


def iota(shape, dim):
    return lax.broadcasted_iota(jnp.int32, shape, dim)


def kernel(
    c_ref,
    left_hbm,
    right_hbm,
    o_ref,
    cz,
    xs,
    xr,
    ye,
    yr,
    yc,
    up,
    r1,
    z1,
    a2,
    pb,
    a3,
    a4,
    z4,
    work,
    waves,
    left,
    right,
    ms,
    mb,
    local_sem,
    table_sem,
    halo_send,
    halo_recv,
    p1_send,
    p1_recv,
    p2a_send,
    p2a_recv,
    p2b_send,
    p2b_recv,
    p3b_send,
    p3b_recv,
    p3a_send,
    p3a_recv,
    p4_send,
    p4_recv,
    m_send,
    m_recv,
):
    gx, gy, gz = lax.axis_index("gx"), lax.axis_index("gy"), lax.axis_index("gz")
    z_chip, x_low = gz // 2, gz % 2
    x_chip, core = (gy // 2) * 2 + x_low, gy % 2
    mine = gy * 8 + gz

    def z_peer(offset):
        dz, dx = offset
        return ((z_chip + dz) % 4) * 2 + (x_low + dx) % 2

    def plane_peer(s):
        k = s % 16
        dx = k % 4
        dz = (k // 4 + dx) % 4
        px, pz, pc = (x_chip + dx) % 4, (z_chip + dz) % 4, (core + s // 16) % 2
        return (px // 2) * 2 + pc, pz * 2 + px % 2

    def remote(src, dst, send, recv, **where):
        return pltpu.make_async_remote_copy(
            src, dst, send, recv, device_id=where, device_id_type=MESH
        )

    def drain(ref, sem):
        pltpu.make_async_copy(ref, ref, sem).wait()

    load = pltpu.make_async_copy(c_ref, cz.at[pl.ds(1, BZ)], local_sem)
    load.start()
    load_left = pltpu.make_async_copy(left_hbm, left, table_sem.at[0])
    load_right = pltpu.make_async_copy(right_hbm, right, table_sem.at[1])
    load_left.start()
    load_right.start()
    barrier = pltpu.get_barrier_semaphore()

    def greet(s, carry):
        a, b = plane_peer(s)
        pl.semaphore_signal(
            barrier, inc=1, device_id={"gy": a, "gz": b}, device_id_type=MESH
        )
        return carry

    lax.fori_loop(1, 32, greet, 0)
    for s in (1, 2, 3):
        pl.semaphore_signal(
            barrier, inc=1, device_id={"gx": (gx + s) % 4}, device_id_type=MESH
        )
    load.wait()

    flat = cz.reshape((BZ + 2) * BX, BY)
    xs[0] = flat[pl.ds(BX, BZ, stride=BX), :]
    xs[1] = flat[pl.ds(BX + BX - 1, BZ, stride=BX), :]
    lane = iota((BX, BY), 1)

    def pack(z, acc):
        turned = pltpu.roll(cz[z + 1], 2 * z, 1)
        keep = (lane == 2 * z) | (lane == (2 * z + BY - 1) % BY)
        return jnp.where(keep, turned, acc)

    ye[...] = lax.fori_loop(0, BZ, pack, jnp.zeros((BX, BY), F32))

    pl.semaphore_wait(barrier, 34)
    halo = [
        remote(c_ref.at[pl.ds(BZ - 1, 1)], cz.at[pl.ds(0, 1)], halo_send.at[0], halo_recv.at[0], gz=(gz + 1) % 8),
        remote(c_ref.at[pl.ds(0, 1)], cz.at[pl.ds(BZ + 1, 1)], halo_send.at[1], halo_recv.at[1], gz=(gz + 7) % 8),
        remote(xs.at[1], xr.at[0], halo_send.at[2], halo_recv.at[2], gx=(gx + 1) % 4),
        remote(xs.at[0], xr.at[1], halo_send.at[3], halo_recv.at[3], gx=(gx + 3) % 4),
        remote(ye, yr.at[0], halo_send.at[4], halo_recv.at[4], gy=(gy + 1) % 4),
        remote(ye, yr.at[1], halo_send.at[5], halo_recv.at[5], gy=(gy + 3) % 4),
    ]
    for copy in halo:
        copy.start()
    for copy in halo:
        copy.wait()
    yc[...] = jnp.where(lane % 2 == 0, pltpu.roll(yr[0], 1, 1), pltpu.roll(yr[1], BY - 1, 1))

    row = iota((BX, BY), 0)

    def terms(c):
        square = c * c
        return square * c - c, 1.05 - square

    def stencil(z, total):
        c = cz[z + 1]
        p, m = terms(c)
        pz, mz = terms(cz[z + 2])
        divergence = (m + mz) * (pz - p)
        pz, mz = terms(cz[z])
        divergence = divergence - (m + mz) * (p - pz)
        ph, mh = terms(jnp.broadcast_to(xr[0, pl.ds(z, 1), :], (BX, BY)))
        pp = jnp.where(row == 0, ph, pltpu.roll(p, 1, 0))
        mp = jnp.where(row == 0, mh, pltpu.roll(m, 1, 0))
        flux = (m + mp) * (p - pp)
        ph, mh = terms(jnp.broadcast_to(xr[1, pl.ds(z, 1), :], (BX, BY)))
        after = jnp.where(row == BX - 1, (m + mh) * (ph - p), pltpu.roll(flux, BX - 1, 0))
        divergence = divergence + (after - flux)
        ph, mh = terms(pltpu.roll(yc[...], (BY - 2 * z) % BY, 1))
        pp = jnp.where(lane == 0, ph, pltpu.roll(p, 1, 1))
        mp = jnp.where(lane == 0, mh, pltpu.roll(m, 1, 1))
        flux = (m + mp) * (p - pp)
        after = jnp.where(lane == BY - 1, (m + mh) * (ph - p), pltpu.roll(flux, BY - 1, 1))
        divergence = divergence + (after - flux)
        up[z] = c + (0.5 * step_length) * divergence
        return total + jnp.sum(m.reshape(16, 8, BY), axis=0)

    def p1_copies(h, start):
        for offset in Z_OFFSETS:
            peer = z_peer(offset)
            rows = pl.ds(pl.multiple_of(peer * 16 + h * 8, 8), 8)
            remote(
                up.at[pl.ds(start, CHUNK), rows, :],
                r1.at[h, pl.ds(gz * BZ + start, CHUNK)],
                p1_send,
                p1_recv.at[h],
                gz=peer,
            ).start()
        rows = pl.ds(pl.multiple_of(gz * 16 + h * 8, 8), 8)
        pltpu.make_async_copy(
            up.at[pl.ds(start, CHUNK), rows, :],
            r1.at[h, pl.ds(gz * BZ + start, CHUNK)],
            p1_recv.at[h],
        ).start()

    def stencil_chunk(k, total):
        start = k * CHUNK
        total = lax.fori_loop(start, start + CHUNK, stencil, total)
        p1_copies(0, start)
        return total

    total = lax.fori_loop(0, BZ // CHUNK, stencil_chunk, jnp.zeros((8, BY), F32))

    def second_half(k, carry):
        p1_copies(1, k * CHUNK)
        return carry

    lax.fori_loop(0, BZ // CHUNK, second_half, 0)

    ms[0] = total
    for s in (1, 2, 3):
        remote(ms.at[0], ms.at[s], m_send.at[0], m_recv.at[0], gx=(gx + s) % 4).start()

    def fill(k, carry):
        rows = pl.ds(pl.multiple_of(k * 32, 32), 32)
        waves[rows, :] = wave_of(iota((32, N), 0) + k * 32) + wave_of(iota((32, N), 1))
        return carry

    lax.fori_loop(0, N // 32, fill, 0)
    load_left.wait()
    load_right.wait()

    drain(ms.at[pl.ds(1, 3)], m_recv.at[0])
    mb[0] = ms[0] + ms[1] + ms[2] + ms[3]

    def spread(s, carry):
        a, b = plane_peer(s)
        remote(mb.at[0], mb.at[s], m_send.at[1], m_recv.at[1], gy=a, gz=b).start()
        return carry

    lax.fori_loop(1, 32, spread, 0)

    def fold(a, b):
        return thirds(a + b, 0), thirds(a - b, 0)

    def z_forward(h):
        source = r1.at[h].reshape(N * 8, BY)
        target = z1.at[h].reshape(N * 8, BY)

        def pair(k, carry):
            x0, x1 = 2 * k, 2 * k + 1

            def rows(base):
                return jnp.concatenate(
                    [
                        source[pl.ds(base * 8 + x0, HALF, stride=8), :],
                        source[pl.ds(base * 8 + x1, HALF, stride=8), :],
                    ],
                    axis=1,
                )

            plus, minus = fold(rows(0), rows(HALF))
            even = matmul(left[0], plus)
            odd = matmul(left[1], minus)
            for base, value in ((0, even), (HALF, odd)):
                target[pl.ds(base * 8 + x0, HALF, stride=8), :] = value[:, :BY]
                target[pl.ds(base * 8 + x1, HALF, stride=8), :] = value[:, BY:]
            return carry

        lax.fori_loop(0, 4, pair, 0)

    def gx_copies(source, target, send, recv, outward):
        for s in (1, 3, 2, 0):
            peer = (gx + s) % 4
            if outward:
                src, dst = source.at[pl.ds(peer * 128, 128)], target.at[gx]
            else:
                src, dst = source.at[peer], target.at[pl.ds(gx * 128, 128)]
            if s:
                remote(src, dst, send, recv, gx=peer).start()
            else:
                pltpu.make_async_copy(src, dst, recv).start()

    for h in (0, 1):
        drain(r1.at[h], p1_recv.at[h])
        z_forward(h)
        gx_copies(z1.at[h], a2.at[h], p2a_send, p2a_recv.at[h], True)

    def plane_part(h, p, a, b):
        rows = pl.ds(pl.multiple_of(b * 16 + h * 8, 8), 8)
        return pb.at[:, p, rows, pl.ds(pl.multiple_of(a * 128, 128), 128)]

    def p2b_copies(h, p):
        def send(s, carry):
            a, b = plane_peer(s)
            src = a2.at[h, :, (a * 8 + b) * 4 + p]
            remote(
                src, plane_part(h, p, gy, gz), p2b_send, p2b_recv.at[h * 4 + p], gy=a, gz=b
            ).start()
            return carry

        lax.fori_loop(1, 32, send, 0)
        pltpu.make_async_copy(
            a2.at[h, :, mine * 4 + p], plane_part(h, p, gy, gz), p2b_recv.at[h * 4 + p]
        ).start()

    def p3b_copies(h, p):
        def send(s, carry):
            a, b = plane_peer(s)
            remote(
                plane_part(h, p, a, b), a3.at[h, :, mine * 4 + p], p3b_send, p3b_recv.at[h], gy=a, gz=b
            ).start()
            return carry

        lax.fori_loop(1, 32, send, 0)
        pltpu.make_async_copy(
            plane_part(h, p, gy, gz), a3.at[h, :, mine * 4 + p], p3b_recv.at[h]
        ).start()

    for h in (0, 1):
        drain(a2.at[h], p2a_recv.at[h])

        def send_planes(p, carry):
            p2b_copies(h, p)
            return carry

        lax.fori_loop(0, 4, send_planes, 0)

    drain(mb.at[pl.ds(1, 31)], m_recv.at[1])
    mobility = jnp.sum(jnp.sum(mb[...], axis=0), keepdims=True)
    factor = (step_length * stiffness) * (mobility / float(N * N * N))

    def plane(p, carry):
        for h in (0, 1):
            drain(pb.at[:, p, pl.ds(0, 64), :], p2b_recv.at[h * 4 + p])
        wave_z = wave_of(gx * 128 + mine * 4 + p)

        def x_forward(k, carry):
            cols = pl.ds(pl.multiple_of(k * HALF, HALF), HALF)
            low = jnp.concatenate([pb[0, p, :, cols], pb[1, p, :, cols]], axis=0)
            high = jnp.concatenate([pb[2, p, :, cols], pb[3, p, :, cols]], axis=0)
            plus, minus = fold(low, high)
            work[pl.ds(0, HALF), cols] = matmul(left[0], plus)
            work[pl.ds(HALF, HALF), cols] = matmul(left[1], minus)
            return carry

        lax.fori_loop(0, 2, x_forward, 0)

        def y_both(k, carry):
            rows = pl.ds(pl.multiple_of(k * 128, 128), 128)
            a, b = work[rows, :HALF], work[rows, HALF:]
            parts = []
            for value, table, back, cols in (
                (a + b, 0, 0, pl.ds(0, HALF)),
                (a - b, 1, 2, pl.ds(HALF, HALF)),
            ):
                value = matmul(thirds(value, 1), right[table])
                wave = waves[rows, cols] + wave_z
                value = value / (1.0 + factor * (wave * wave))
                parts.append(matmul(thirds(value, 1), right[back]))
            work[rows, :HALF] = parts[0] + parts[1]
            work[rows, HALF:] = parts[0] - parts[1]
            return carry

        lax.fori_loop(0, 4, y_both, 0)

        def x_inverse(k, carry):
            cols = pl.ds(pl.multiple_of(k * HALF, HALF), HALF)
            a = matmul(left[0], thirds(work[pl.ds(0, HALF), cols], 0))
            b = matmul(left[2], thirds(work[pl.ds(HALF, HALF), cols], 0))
            plus, minus = a + b, a - b
            pb[0, p, :, cols], pb[1, p, :, cols] = plus[:128], plus[128:]
            pb[2, p, :, cols], pb[3, p, :, cols] = minus[:128], minus[128:]
            return carry

        lax.fori_loop(0, 2, x_inverse, 0)
        p3b_copies(0, p)
        return carry

    lax.fori_loop(0, 4, plane, 0)

    def rest(p, carry):
        p3b_copies(1, p)
        return carry

    lax.fori_loop(0, 4, rest, 0)

    for h in (0, 1):
        drain(a3.at[h], p3b_recv.at[h])
        gx_copies(a3.at[h], a4.at[h], p3a_send, p3a_recv.at[h], False)

    def z_inverse(h):
        source = a4.at[h].reshape(N * 8, BY)
        target = z4.at[h].reshape(N * 8, BY)

        def pair(k, carry):
            x0, x1 = 2 * k, 2 * k + 1

            def rows(base):
                return jnp.concatenate(
                    [
                        source[pl.ds(base * 8 + x0, HALF, stride=8), :],
                        source[pl.ds(base * 8 + x1, HALF, stride=8), :],
                    ],
                    axis=1,
                )

            a = matmul(left[0], thirds(rows(0), 0))
            b = matmul(left[2], thirds(rows(HALF), 0))
            for base, value in ((0, a + b), (HALF, a - b)):
                target[pl.ds(base * 8 + x0, HALF, stride=8), :] = value[:, :BY]
                target[pl.ds(base * 8 + x1, HALF, stride=8), :] = value[:, BY:]
            return carry

        lax.fori_loop(0, 4, pair, 0)

    for h in (0, 1):
        drain(a4.at[h], p3a_recv.at[h])
        z_inverse(h)
        rows = pl.ds(pl.multiple_of(gz * 16 + h * 8, 8), 8)

        def back(k, carry):
            start = k * CHUNK
            for offset in Z_OFFSETS:
                peer = z_peer(offset)
                remote(
                    z4.at[h, pl.ds(peer * BZ + start, CHUNK)],
                    o_ref.at[pl.ds(start, CHUNK), rows, :],
                    p4_send,
                    p4_recv.at[h],
                    gz=peer,
                ).start()
            pltpu.make_async_copy(
                z4.at[h, pl.ds(gz * BZ + start, CHUNK)],
                o_ref.at[pl.ds(start, CHUNK), rows, :],
                p4_recv.at[h],
            ).start()
            return carry

        lax.fori_loop(0, BZ // CHUNK, back, 0)

    for h in (0, 1):
        drain(o_ref.at[pl.ds(0, 32)], p4_recv.at[h])
    drain(up.at[pl.ds(0, 56)], p1_send)
    drain(ms.at[pl.ds(1, 3)], m_send.at[0])
    drain(mb.at[pl.ds(1, 31)], m_send.at[1])
    drain(z1.at[:, pl.ds(0, 384)], p2a_send)
    drain(up.at[pl.ds(0, 62)], p2b_send)
    drain(up.at[pl.ds(0, 62)], p3b_send)
    drain(z1.at[:, pl.ds(0, 384)], p3a_send)
    drain(up.at[pl.ds(0, 56)], p4_send)


def local(concentration):
    left, right = tables()
    vmem, dma = pltpu.VMEM, pltpu.SemaphoreType.DMA
    any_space = pl.BlockSpec(memory_space=pl.ANY)
    return pl.pallas_call(
        kernel,
        out_shape=jax.ShapeDtypeStruct((BZ, BX, BY), F32),
        in_specs=[any_space] * 3,
        out_specs=any_space,
        scratch_shapes=[
            vmem((BZ + 2, BX, BY), F32),
            vmem((2, BZ, BY), F32),
            vmem((2, BZ, BY), F32),
            vmem((BX, BY), F32),
            vmem((2, BX, BY), F32),
            vmem((BX, BY), F32),
            vmem((BZ, BX, BY), F32),
            vmem((2, N, 8, BY), F32),
            vmem((2, N, 8, BY), F32),
            vmem((2, 4, 128, 8, BY), F32),
            vmem((4, 4, BX, N), F32),
            vmem((2, 4, 128, 8, BY), F32),
            vmem((2, N, 8, BY), F32),
            vmem((2, N, 8, BY), F32),
            vmem((N, N), F32),
            vmem((N, N), F32),
            vmem((3, HALF, 3 * HALF), BF16),
            vmem((3, 3 * HALF, HALF), BF16),
            vmem((4, 8, BY), F32),
            vmem((32, 8, BY), F32),
            dma,
            dma((2,)),
            dma((6,)),
            dma((6,)),
            dma,
            dma((2,)),
            dma,
            dma((2,)),
            dma,
            dma((8,)),
            dma,
            dma((2,)),
            dma,
            dma((2,)),
            dma,
            dma((2,)),
            dma((2,)),
            dma((2,)),
        ],
        compiler_params=pltpu.CompilerParams(
            collective_id=0, has_side_effects=True, vmem_limit_bytes=60 * 2**20
        ),
    )(concentration, jnp.asarray(left), jnp.asarray(right))


def solution(mesh):
    spec = P("gz", "gx", "gy")
    return jax.shard_map(local, mesh=mesh, in_specs=(spec,), out_specs=spec, check_vma=False)
```

```python
import functools

import jax
import jax.numpy as jnp
import numpy as np
from jax import lax
from jax.experimental import pallas as pl
from jax.experimental.pallas import tpu as pltpu
from jax.sharding import PartitionSpec as P

MESH = pl.DeviceIdType.MESH
F32, BF16 = jnp.float32, jnp.bfloat16

step_length = 0.2
stiffness = 0.25

N = 512
HALF = N // 2
BZ, BX, BY = 64, 128, 128
CHUNKS = 4
X_OFFSETS = ((1, 0), (3, 0), (2, 0), (1, 1), (3, 1), (2, 1), (0, 1))


def split_table(matrix):
    high = matrix.astype(np.float32).astype(jnp.bfloat16)
    low = (matrix - high.astype(np.float64)).astype(np.float32).astype(jnp.bfloat16)
    return high, low


def tables():
    index = np.arange(N)
    angle = 2.0 * np.pi / N * (index[:, None] * index[None, :] % N)
    hartley = (np.cos(angle) + np.sin(angle)) / np.sqrt(N)
    even, odd = hartley[0::2, :HALF], hartley[1::2, :HALF]
    left, right = [], []
    for matrix in (even, odd, odd.T):
        high, low = split_table(matrix)
        left.append(np.concatenate([high, low, high], axis=1))
    for matrix in (even, odd.T, odd):
        high, low = split_table(matrix)
        right.append(np.concatenate([high, low, high], axis=0))
    return np.stack(left), np.stack(right)


def thirds(a, axis):
    high = a.astype(BF16)
    low = (a - high.astype(F32)).astype(BF16)
    return jnp.concatenate([high, high, low], axis=axis)


def matmul(a, b):
    return jnp.dot(a, b, preferred_element_type=F32)


def wave_of(position):
    true = jnp.where(position < HALF, 2 * position, 2 * position - (N - 1))
    folded = jnp.minimum(true, N - true).astype(F32)
    wave = (2.0 * np.pi / N) * folded
    return wave * wave


def iota(shape, dim):
    return lax.broadcasted_iota(jnp.int32, shape, dim)


def kernel(
    c_ref,
    left_hbm,
    right_hbm,
    o_ref,
    cz,
    xs,
    xr,
    ye,
    yr,
    yc,
    up,
    xa,
    ya,
    yb,
    xb,
    zb,
    ya2,
    xb2,
    xa2,
    yb2,
    waves,
    left,
    right,
    ms,
    mb,
    local_sem,
    table_sem,
    halo_send,
    halo_recv,
    sent,
    xa_sem,
    ya_sem,
    yb_sem,
    xb_sem,
    zb_sem,
    ya2_sem,
    xb2_sem,
    xa2_sem,
    yb2_sem,
    out_sem,
    m_send,
    m_recv,
):
    gx, gy, gz = lax.axis_index("gx"), lax.axis_index("gy"), lax.axis_index("gz")
    z_chip, x_low = gz // 2, gz % 2
    x_chip, core = (gy // 2) * 2 + x_low, gy % 2
    mine = gy * 2 + x_low

    def plane_peer(s):
        k = s % 16
        dx = k % 4
        dz = (k // 4 + dx) % 4
        px, pz, pc = (x_chip + dx) % 4, (z_chip + dz) % 4, (core + s // 16) % 2
        return (px // 2) * 2 + pc, pz * 2 + px % 2

    def row_peer(offset):
        px, pc = (x_chip + offset[0]) % 4, (core + offset[1]) % 2
        return (px // 2) * 2 + pc, px % 2

    def side_peer(s):
        dy = s % 4
        return (gx + dy) % 4, (z_chip + s // 4 + dy) % 4

    def remote(src, dst, send, recv, **where):
        return pltpu.make_async_remote_copy(
            src, dst, send, recv, device_id=where, device_id_type=MESH
        )

    def here(src, dst, recv):
        pltpu.make_async_copy(src, dst, recv).start()

    def drain(ref, sem):
        pltpu.make_async_copy(ref, ref, sem).wait()

    def lanes(block):
        return pl.ds(pl.multiple_of(block * 128, 128), 128)

    def rows(start, size):
        return pl.ds(pl.multiple_of(start, size), size)

    load = pltpu.make_async_copy(c_ref, cz.at[pl.ds(1, BZ)], local_sem)
    load.start()
    load_left = pltpu.make_async_copy(left_hbm, left, table_sem.at[0])
    load_right = pltpu.make_async_copy(right_hbm, right, table_sem.at[1])
    load_left.start()
    load_right.start()
    barrier = pltpu.get_barrier_semaphore()

    def greet(s, carry):
        a, b = plane_peer(s)
        pl.semaphore_signal(
            barrier, inc=1, device_id={"gy": a, "gz": b}, device_id_type=MESH
        )
        return carry

    def greet_side(s, carry):
        a, b = side_peer(s)
        pl.semaphore_signal(
            barrier, inc=1, device_id={"gx": a, "gz": b * 2 + x_low}, device_id_type=MESH
        )
        return carry

    lax.fori_loop(1, 32, greet, 0)
    lax.fori_loop(1, 16, greet_side, 0)
    load.wait()

    flat = cz.reshape((BZ + 2) * BX, BY)
    xs[0] = flat[pl.ds(BX, BZ, stride=BX), :]
    xs[1] = flat[pl.ds(BX + BX - 1, BZ, stride=BX), :]
    lane = iota((BX, BY), 1)

    def pack(z, acc):
        turned = pltpu.roll(cz[z + 1], 2 * z, 1)
        keep = (lane == 2 * z) | (lane == (2 * z + BY - 1) % BY)
        return jnp.where(keep, turned, acc)

    ye[...] = lax.fori_loop(0, BZ, pack, jnp.zeros((BX, BY), F32))

    pl.semaphore_wait(barrier, 46)
    halo = [
        remote(c_ref.at[pl.ds(BZ - 1, 1)], cz.at[pl.ds(0, 1)], halo_send.at[0], halo_recv.at[0], gz=(gz + 1) % 8),
        remote(c_ref.at[pl.ds(0, 1)], cz.at[pl.ds(BZ + 1, 1)], halo_send.at[1], halo_recv.at[1], gz=(gz + 7) % 8),
        remote(xs.at[1], xr.at[0], halo_send.at[2], halo_recv.at[2], gx=(gx + 1) % 4),
        remote(xs.at[0], xr.at[1], halo_send.at[3], halo_recv.at[3], gx=(gx + 3) % 4),
        remote(ye, yr.at[0], halo_send.at[4], halo_recv.at[4], gy=(gy + 1) % 4),
        remote(ye, yr.at[1], halo_send.at[5], halo_recv.at[5], gy=(gy + 3) % 4),
    ]
    for copy in halo:
        copy.start()
    for copy in halo:
        copy.wait()
    yc[...] = jnp.where(lane % 2 == 0, pltpu.roll(yr[0], 1, 1), pltpu.roll(yr[1], BY - 1, 1))

    row = iota((BX, BY), 0)

    def terms(c):
        square = c * c
        return square * c - c, 1.05 - square

    def stencil(z, total):
        c = cz[z + 1]
        p, m = terms(c)
        pz, mz = terms(cz[z + 2])
        divergence = (m + mz) * (pz - p)
        pz, mz = terms(cz[z])
        divergence = divergence - (m + mz) * (p - pz)
        ph, mh = terms(jnp.broadcast_to(xr[0, pl.ds(z, 1), :], (BX, BY)))
        pp = jnp.where(row == 0, ph, pltpu.roll(p, 1, 0))
        mp = jnp.where(row == 0, mh, pltpu.roll(m, 1, 0))
        flux = (m + mp) * (p - pp)
        ph, mh = terms(jnp.broadcast_to(xr[1, pl.ds(z, 1), :], (BX, BY)))
        after = jnp.where(row == BX - 1, (m + mh) * (ph - p), pltpu.roll(flux, BX - 1, 0))
        divergence = divergence + (after - flux)
        ph, mh = terms(pltpu.roll(yc[...], (BY - 2 * z) % BY, 1))
        pp = jnp.where(lane == 0, ph, pltpu.roll(p, 1, 1))
        mp = jnp.where(lane == 0, mh, pltpu.roll(m, 1, 1))
        flux = (m + mp) * (p - pp)
        after = jnp.where(lane == BY - 1, (m + mh) * (ph - p), pltpu.roll(flux, BY - 1, 1))
        divergence = divergence + (after - flux)
        up[z] = c + (0.5 * step_length) * divergence
        return total + jnp.sum(m.reshape(16, 8, BY), axis=0)

    def gx_copies(source, target, send, recv):
        for s in (1, 3, 2, 0):
            peer = (gx + s) % 4
            if s:
                remote(source(peer), target, sent.at[send], recv, gx=peer).start()
            else:
                here(source(gx), target, recv)

    def row_copies(source, target, send, recv):
        for offset in X_OFFSETS:
            a, low = row_peer(offset)
            remote(
                source(a, low), target, sent.at[send], recv, gy=a, gz=z_chip * 2 + low
            ).start()
        here(source(gy, x_low), target, recv)

    def first(k):
        gx_copies(
            lambda a: up.at[pl.ds(8 * k + 2 * a, 2)],
            xa.at[k, :, rows(gx * 128, 128), :],
            0,
            xa_sem.at[k],
        )
        row_copies(
            lambda a, low: up.at[32 + 8 * k + 2 * a + low],
            yb.at[k, x_low, :, lanes(gy)],
            1,
            yb_sem.at[k],
        )

    def second_a(k):
        row_copies(
            lambda a, low: xa.at[k, :, rows((2 * a + low) * 64, 64), :],
            ya.at[k, x_low, :, :, lanes(gy)],
            2,
            ya_sem.at[k],
        )

    def second_b(k):
        gx_copies(
            lambda a: yb.at[k, :, :, lanes(a)],
            xb.at[k, :, rows(gx * 128, 128), :],
            3,
            xb_sem.at[k],
        )

    def third_a(k):
        def part(h):
            def source(y, z):
                return ya.at[k, :, :, rows(16 * z + 8 * h, 8), lanes(y)]

            target = zb.at[h, pl.ds(2 * z_chip, 2), pl.ds(8 * k + 2 * gx, 2)]

            def send(s, carry):
                y, z = side_peer(s)
                remote(
                    source(y, z), target, sent.at[4], zb_sem.at[h], gx=y, gz=z * 2 + x_low
                ).start()
                return carry

            lax.fori_loop(1, 16, send, 0)
            here(source(gx, z_chip), target, zb_sem.at[h])

        part(0)
        part(1)

    def third_b(k):
        def part(h):
            def source(a, b):
                return xb.at[k, :, rows((2 * a + b % 2) * 64 + 16 * (b // 2) + 8 * h, 8), :]

            target = zb.at[h, pl.ds(2 * z_chip, 2), 32 + 8 * k + mine]

            def send(s, carry):
                a, b = plane_peer(s)
                remote(source(a, b), target, sent.at[5], zb_sem.at[h], gy=a, gz=b).start()
                return carry

            lax.fori_loop(1, 32, send, 0)
            here(source(gy, gz), target, zb_sem.at[h])

        part(0)
        part(1)

    def back_third(k, h):
        def source_a(y, z):
            return zb.at[h, pl.ds(2 * z, 2), pl.ds(8 * k + 2 * y, 2)]

        target_a = ya2.at[k, :, :, rows(16 * z_chip + 8 * h, 8), lanes(gx)]

        def send_a(s, carry):
            y, z = side_peer(s)
            remote(
                source_a(y, z), target_a, sent.at[6], ya2_sem.at[k], gx=y, gz=z * 2 + x_low
            ).start()
            return carry

        def source_b(a, b):
            return zb.at[h, pl.ds(2 * (b // 2), 2), 32 + 8 * k + 2 * a + b % 2]

        target_b = xb2.at[k, :, rows(mine * 64 + 16 * z_chip + 8 * h, 8), :]

        def send_b(s, carry):
            a, b = plane_peer(s)
            remote(source_b(a, b), target_b, sent.at[7], xb2_sem.at[k], gy=a, gz=b).start()
            return carry

        lax.fori_loop(1, 16, send_a, 0)
        here(source_a(gx, z_chip), target_a, ya2_sem.at[k])
        lax.fori_loop(1, 32, send_b, 0)
        here(source_b(gy, gz), target_b, xb2_sem.at[k])

    def back_second_a(k):
        row_copies(
            lambda a, low: ya2.at[k, low, :, :, lanes(a)],
            xa2.at[k, :, rows(mine * 64, 64), :],
            8,
            xa2_sem.at[k],
        )

    def back_second_b(k):
        gx_copies(
            lambda a: xb2.at[k, :, rows(a * 128, 128), :],
            yb2.at[k, :, :, lanes(gx)],
            9,
            yb2_sem.at[k],
        )

    def back_first_a(k):
        gx_copies(
            lambda a: xa2.at[k, :, rows(a * 128, 128), :],
            o_ref.at[pl.ds(8 * k + 2 * gx, 2)],
            10,
            out_sem,
        )

    def back_first_b(k):
        row_copies(
            lambda a, low: yb2.at[k, low, :, lanes(a)],
            o_ref.at[32 + 8 * k + mine],
            11,
            out_sem,
        )

    def x_pass(ref, inverse):
        low = jnp.concatenate([ref[0, :HALF], ref[1, :HALF]], axis=1)
        high = jnp.concatenate([ref[0, HALF:], ref[1, HALF:]], axis=1)
        if inverse:
            even = matmul(left[0], thirds(low, 0))
            odd = matmul(left[2], thirds(high, 0))
            low, high = even + odd, even - odd
        else:
            plus, minus = thirds(low + high, 0), thirds(low - high, 0)
            low, high = matmul(left[0], plus), matmul(left[1], minus)
        ref[0, :HALF], ref[1, :HALF] = low[:, :BY], low[:, BY:]
        ref[0, HALF:], ref[1, HALF:] = high[:, :BY], high[:, BY:]

    def y_pass(ref, inverse):
        flat = ref.reshape(256, N)

        def block(i, carry):
            part = rows(i * 128, 128)
            low, high = flat[part, :HALF], flat[part, HALF:]
            if inverse:
                even = matmul(thirds(low, 1), right[0])
                odd = matmul(thirds(high, 1), right[2])
                low, high = even + odd, even - odd
            else:
                plus, minus = thirds(low + high, 1), thirds(low - high, 1)
                low, high = matmul(plus, right[0]), matmul(minus, right[1])
            flat[part, :HALF] = low
            flat[part, HALF:] = high
            return carry

        lax.fori_loop(0, 2, block, 0)

    def stencil_chunk(k, total):
        total = lax.fori_loop(8 * k, 8 * k + 8, stencil, total)
        total = lax.fori_loop(32 + 8 * k, 40 + 8 * k, stencil, total)

        @pl.when(k < 2)
        def _():
            first(k)

        return total

    ms[0] = lax.fori_loop(0, CHUNKS, stencil_chunk, jnp.zeros((8, BY), F32))

    for s in (1, 2, 3):
        remote(ms.at[0], ms.at[s], m_send.at[0], m_recv.at[0], gx=(gx + s) % 4).start()

    def fill(k, carry):
        part = rows(k * 32, 32)
        waves[part, :] = wave_of(iota((32, BY), 0) + k * 32) + wave_of(iota((32, BY), 1) + gx * BY)
        return carry

    lax.fori_loop(0, N // 32, fill, 0)
    load_left.wait()
    load_right.wait()

    drain(ms.at[pl.ds(1, 3)], m_recv.at[0])
    mb[0] = ms[0] + ms[1] + ms[2] + ms[3]

    def spread(s, carry):
        a, b = plane_peer(s)
        remote(mb.at[0], mb.at[s], m_send.at[1], m_recv.at[1], gy=a, gz=b).start()
        return carry

    lax.fori_loop(1, 32, spread, 0)

    def forward(k, carry):
        @pl.when(k < CHUNKS)
        def _():
            drain(yb.at[k], yb_sem.at[k])
            y_pass(yb.at[k], False)
            second_b(k)
            drain(xa.at[k], xa_sem.at[k])
            x_pass(xa.at[k], False)
            second_a(k)

        @pl.when(k < CHUNKS - 2)
        def _():
            first(k + 2)

        @pl.when(k > 0)
        def _():
            drain(xb.at[k - 1], xb_sem.at[k - 1])
            x_pass(xb.at[k - 1], False)
            third_b(k - 1)
            drain(ya.at[k - 1], ya_sem.at[k - 1])
            y_pass(ya.at[k - 1], False)
            third_a(k - 1)

        return carry

    lax.fori_loop(0, CHUNKS + 1, forward, 0)

    drain(mb.at[pl.ds(1, 31)], m_recv.at[1])
    mobility = jnp.sum(jnp.sum(mb[...], axis=0), keepdims=True)
    factor = (step_length * stiffness) * (mobility / float(N * N * N))

    def z_stage(h):
        drain(zb.at[h], zb_sem.at[h])
        field = zb.at[h].reshape(N * 8, BY)

        def pair(i, carry):
            x0, x1 = 2 * i, 2 * i + 1

            def take(base):
                return jnp.concatenate(
                    [
                        field[pl.ds(base * 8 + x0, HALF, stride=8), :],
                        field[pl.ds(base * 8 + x1, HALF, stride=8), :],
                    ],
                    axis=1,
                )

            position = mine * 64 + 16 * z_chip + 8 * h
            wave0, wave1 = wave_of(position + x0), wave_of(position + x1)
            low, high = take(0), take(HALF)
            parts = []
            for value, table, back, base in (
                (low + high, 0, 0, 0),
                (low - high, 1, 2, HALF),
            ):
                value = matmul(left[table], thirds(value, 0))
                wave = waves[pl.ds(base, HALF), :]
                wave = jnp.concatenate([wave + wave0, wave + wave1], axis=1)
                value = value / (1.0 + factor * (wave * wave))
                parts.append(matmul(left[back], thirds(value, 0)))
            for base, value in ((0, parts[0] + parts[1]), (HALF, parts[0] - parts[1])):
                field[pl.ds(base * 8 + x0, HALF, stride=8), :] = value[:, :BY]
                field[pl.ds(base * 8 + x1, HALF, stride=8), :] = value[:, BY:]
            return carry

        lax.fori_loop(0, 4, pair, 0)
        back_third(0, h)

    z_stage(0)
    z_stage(1)
    back_third(1, 0)
    back_third(1, 1)

    def inverse(k, carry):
        @pl.when(k < CHUNKS)
        def _():
            drain(ya2.at[k], ya2_sem.at[k])
            y_pass(ya2.at[k], True)
            back_second_a(k)
            drain(xb2.at[k], xb2_sem.at[k])
            x_pass(xb2.at[k], True)
            back_second_b(k)

        @pl.when(k < CHUNKS - 2)
        def _():
            back_third(k + 2, 0)
            back_third(k + 2, 1)

        @pl.when(k > 0)
        def _():
            drain(xa2.at[k - 1], xa2_sem.at[k - 1])
            x_pass(xa2.at[k - 1], True)
            back_first_a(k - 1)
            drain(yb2.at[k - 1], yb2_sem.at[k - 1])
            y_pass(yb2.at[k - 1], True)
            back_first_b(k - 1)

        return carry

    lax.fori_loop(0, CHUNKS + 1, inverse, 0)
    drain(o_ref, out_sem)

    for i, layers in enumerate((24, 28, 28, 24, 30, 31, 30, 31, 28, 24, 24, 28)):
        drain(up.at[pl.ds(0, layers)], sent.at[i])
    drain(ms.at[pl.ds(1, 3)], m_send.at[0])
    drain(mb.at[pl.ds(1, 31)], m_send.at[1])


def local(concentration):
    left, right = tables()
    vmem, dma = pltpu.VMEM, pltpu.SemaphoreType.DMA
    any_space = pl.BlockSpec(memory_space=pl.ANY)
    x_field = vmem((CHUNKS, 2, N, BY), F32)
    ya_field = vmem((CHUNKS, 2, 2, 64, N), F32)
    yb_field = vmem((CHUNKS, 2, BX, N), F32)
    return pl.pallas_call(
        kernel,
        out_shape=jax.ShapeDtypeStruct((BZ, BX, BY), F32),
        in_specs=[any_space] * 3,
        out_specs=any_space,
        scratch_shapes=[
            vmem((BZ + 2, BX, BY), F32),
            vmem((2, BZ, BY), F32),
            vmem((2, BZ, BY), F32),
            vmem((BX, BY), F32),
            vmem((2, BX, BY), F32),
            vmem((BX, BY), F32),
            vmem((BZ, BX, BY), F32),
            x_field,
            ya_field,
            yb_field,
            x_field,
            vmem((2, 8, BZ, 8, BY), F32),
            ya_field,
            x_field,
            x_field,
            yb_field,
            vmem((N, BY), F32),
            vmem((3, HALF, 3 * HALF), BF16),
            vmem((3, 3 * HALF, HALF), BF16),
            vmem((4, 8, BY), F32),
            vmem((32, 8, BY), F32),
            dma,
            dma((2,)),
            dma((6,)),
            dma((6,)),
            dma((12,)),
            dma((CHUNKS,)),
            dma((CHUNKS,)),
            dma((CHUNKS,)),
            dma((CHUNKS,)),
            dma((2,)),
            dma((CHUNKS,)),
            dma((CHUNKS,)),
            dma((CHUNKS,)),
            dma((CHUNKS,)),
            dma,
            dma((2,)),
            dma((2,)),
        ],
        compiler_params=pltpu.CompilerParams(
            collective_id=0, has_side_effects=True, vmem_limit_bytes=60 * 2**20
        ),
    )(concentration, jnp.asarray(left), jnp.asarray(right))


def solution(mesh):
    spec = P("gz", "gx", "gy")
    return jax.shard_map(local, mesh=mesh, in_specs=(spec,), out_specs=spec, check_vma=False)
```

```python
import functools

import jax
import jax.numpy as jnp
import numpy as np
from jax import lax
from jax.experimental import pallas as pl
from jax.experimental.pallas import tpu as pltpu
from jax.sharding import PartitionSpec as P

MESH = pl.DeviceIdType.MESH
F32, BF16 = jnp.float32, jnp.bfloat16

step_length = 0.2
stiffness = 0.25

N = 512
HALF = N // 2
BZ, BX, BY = 64, 128, 128
CHUNKS = 4
FORWARD = (
    ("F", 0), ("F", 1), ("I", 2), ("I", 3), ("G", 0), ("P", 0), ("S", 0), ("F", 2), ("S", 1),
    ("M", 0), ("H", 0), ("F", 3), ("T", 0), ("S", 2), ("T", 1), ("S", 3), ("T", 2), ("T", 3),
)
BACKWARD = (
    ("Z", 0), ("Z", 1), ("T", 1), ("S", 0), ("T", 2), ("S", 1), ("T", 3), ("F", 0), ("S", 2),
    ("F", 1), ("S", 3), ("F", 2), ("F", 3),
)
X_OFFSETS = ((1, 0), (3, 0), (2, 0), (1, 1), (3, 1), (2, 1), (0, 1))


def split_table(matrix):
    high = matrix.astype(np.float32).astype(jnp.bfloat16)
    low = (matrix - high.astype(np.float64)).astype(np.float32).astype(jnp.bfloat16)
    return high, low


def tables():
    index = np.arange(N)
    angle = 2.0 * np.pi / N * (index[:, None] * index[None, :] % N)
    hartley = (np.cos(angle) + np.sin(angle)) / np.sqrt(N)
    even, odd = hartley[0::2, :HALF], hartley[1::2, :HALF]
    left, right = [], []
    for matrix in (even, odd, odd.T):
        high, low = split_table(matrix)
        left.append(np.concatenate([high, low], axis=1))
    for matrix in (even, odd.T, odd):
        high, low = split_table(matrix)
        right.append(np.concatenate([high, low], axis=0))
    return np.stack(left), np.stack(right)


def thirds(a, axis):
    high = a.astype(BF16)
    low = (a - high.astype(F32)).astype(BF16)
    return jnp.concatenate([high, high, low], axis=axis)


def matmul(a, b):
    return jnp.dot(a, b, preferred_element_type=F32)


def wave_of(position):
    true = jnp.where(position < HALF, 2 * position, 2 * position - (N - 1))
    folded = jnp.minimum(true, N - true).astype(F32)
    wave = (2.0 * np.pi / N) * folded
    return wave * wave


def iota(shape, dim):
    return lax.broadcasted_iota(jnp.int32, shape, dim)


def kernel(
    c_ref,
    left_hbm,
    right_hbm,
    o_ref,
    cz,
    xs,
    xr,
    ye,
    yr,
    yc,
    zr,
    up,
    xa,
    ya,
    yb,
    xb,
    zb,
    ya2,
    xb2,
    xa2,
    yb2,
    waves,
    left,
    right,
    ms,
    mb,
    local_sem,
    table_sem,
    halo_send,
    halo_recv,
    sent,
    xa_sem,
    ya_sem,
    yb_sem,
    xb_sem,
    zb_sem,
    ya2_sem,
    xb2_sem,
    xa2_sem,
    yb2_sem,
    out_sem,
    m_send,
    m_recv,
    ready,
):
    gx, gy, gz = lax.axis_index("gx"), lax.axis_index("gy"), lax.axis_index("gz")
    z_chip, x_low = gz // 2, gz % 2
    x_chip, core = (gy // 2) * 2 + x_low, gy % 2
    mine = gy * 2 + x_low

    def plane_peer(s):
        k = s % 16
        dx = k % 4
        dz = (k // 4 + dx) % 4
        px, pz, pc = (x_chip + dx) % 4, (z_chip + dz) % 4, (core + s // 16) % 2
        return (px // 2) * 2 + pc, pz * 2 + px % 2

    def row_peer(offset):
        px, pc = (x_chip + offset[0]) % 4, (core + offset[1]) % 2
        return (px // 2) * 2 + pc, px % 2

    def side_peer(s):
        dy = s % 4
        return (gx + dy) % 4, (z_chip + s // 4 + dy) % 4

    def remote(src, dst, send, recv, **where):
        return pltpu.make_async_remote_copy(
            src, dst, send, recv, device_id=where, device_id_type=MESH
        )

    def here(src, dst, recv):
        pltpu.make_async_copy(src, dst, recv).start()

    def drain(ref, sem):
        pltpu.make_async_copy(ref, ref, sem).wait()

    def lanes(block):
        return pl.ds(pl.multiple_of(block * 128, 128), 128)

    def rows(start, size):
        return pl.ds(pl.multiple_of(start, size), size)

    load = pltpu.make_async_copy(c_ref, cz, local_sem)
    load.start()
    pair, third = pl.ds(0, N), pl.ds(N, HALF)
    loads = [
        pltpu.make_async_copy(left_hbm, left.at[:, :, pair], table_sem.at[0]),
        pltpu.make_async_copy(left_hbm.at[:, :, pl.ds(0, HALF)], left.at[:, :, third], table_sem.at[1]),
        pltpu.make_async_copy(right_hbm, right.at[:, pair], table_sem.at[2]),
        pltpu.make_async_copy(right_hbm.at[:, pl.ds(0, HALF)], right.at[:, third], table_sem.at[3]),
    ]
    for copy in loads:
        copy.start()
    barrier = pltpu.get_barrier_semaphore()

    for offset in X_OFFSETS:
        a, low = row_peer(offset)
        pl.semaphore_signal(
            barrier, inc=1, device_id={"gy": a, "gz": z_chip * 2 + low}, device_id_type=MESH
        )
    across = ((z_chip + 3 - 2 * x_low) % 4) * 2 + 1 - x_low
    columns = [((z_chip + s) % 4) * 2 + x_low for s in (1, 2, 3)]
    for s in (1, 2, 3):
        pl.semaphore_signal(
            barrier, inc=1, device_id={"gx": (gx + s) % 4}, device_id_type=MESH
        )
    for other in columns + [across]:
        pl.semaphore_signal(barrier, inc=1, device_id={"gz": other}, device_id_type=MESH)
    load.wait()

    flat = cz.reshape(BZ * BX, BY)
    xs[0] = flat[pl.ds(0, BZ, stride=BX), :]
    xs[1] = flat[pl.ds(BX - 1, BZ, stride=BX), :]
    lane = iota((BX, BY), 1)
    row = iota((BX, BY), 0)

    def pack(z, acc):
        turned = pltpu.roll(cz[z], 2 * z, 1)
        keep = (lane == 2 * z) | (lane == (2 * z + BY - 1) % BY)
        return jnp.where(keep, turned, acc)

    ye[...] = lax.fori_loop(0, BZ, pack, jnp.zeros((BX, BY), F32), unroll=4)

    def terms(c):
        square = c * c
        return square * c - c, 1.05 - square

    def inner(z, total):
        c = cz[z]
        p, m = terms(c)
        pz, mz = terms(cz[jnp.minimum(z + 1, BZ - 1)])
        divergence = (m + mz) * (pz - p)
        pz, mz = terms(cz[jnp.maximum(z - 1, 0)])
        divergence = divergence - (m + mz) * (p - pz)
        before = jnp.where(row == 0, p, pltpu.roll(p, 1, 0))
        flux = (m + pltpu.roll(m, 1, 0)) * (p - before)
        divergence = divergence + (pltpu.roll(flux, BX - 1, 0) - flux)
        before = jnp.where(lane == 0, p, pltpu.roll(p, 1, 1))
        flux = (m + pltpu.roll(m, 1, 1)) * (p - before)
        divergence = divergence + (pltpu.roll(flux, BY - 1, 1) - flux)
        up[z] = c + (0.5 * step_length) * divergence
        return total + jnp.sum(m.reshape(16, 8, BY), axis=0)

    def inner_chunk(k):
        total = lax.fori_loop(8 * k, 8 * k + 8, inner, jnp.zeros((8, BY), F32), unroll=2)
        total = lax.fori_loop(32 + 8 * k, 40 + 8 * k, inner, total, unroll=2)
        ms[0] = total if k == 0 else ms[0] + total

    pl.semaphore_wait(barrier, 14)
    halo = [
        remote(ye, yr.at[0], halo_send.at[4], halo_recv.at[4], gy=(gy + 1) % 4),
        remote(ye, yr.at[1], halo_send.at[5], halo_recv.at[5], gy=(gy + 3) % 4),
        remote(c_ref.at[BZ - 1], zr.at[0], halo_send.at[0], halo_recv.at[0], gz=(gz + 1) % 8),
        remote(c_ref.at[0], zr.at[1], halo_send.at[1], halo_recv.at[1], gz=(gz + 7) % 8),
        remote(xs.at[1], xr.at[0], halo_send.at[2], halo_recv.at[2], gx=(gx + 1) % 4),
        remote(xs.at[0], xr.at[1], halo_send.at[3], halo_recv.at[3], gx=(gx + 3) % 4),
    ]
    for copy in halo:
        copy.start()
    inner_chunk(0)
    inner_chunk(1)
    for copy in halo:
        copy.wait()

    def inflow(inside, outside):
        p, m = terms(inside)
        ph, mh = terms(outside)
        return (0.5 * step_length) * ((m + mh) * (ph - p))

    yc[...] = inflow(
        ye[...], jnp.where(lane % 2 == 0, pltpu.roll(yr[0], 1, 1), pltpu.roll(yr[1], BY - 1, 1))
    )
    xr[0] = inflow(xs[0], xr[0])
    xr[1] = inflow(xs[1], xr[1])
    edge = (lane == 0) | (lane == BY - 1)
    layers = up.reshape(BZ * BX, BY)

    def outer(z, carry):
        turned = pltpu.roll(yc[...], (BY - 2 * z) % BY, 1)
        up[z] = up[z] + jnp.where(edge, turned, 0.0)
        return carry

    def outer_chunk(k):
        if k == 0:
            up[0] = up[0] + inflow(cz[0], zr[0])
        if k == CHUNKS - 1:
            up[BZ - 1] = up[BZ - 1] + inflow(cz[BZ - 1], zr[1])
        for base in (8 * k, 32 + 8 * k):
            for side, place in ((0, 0), (1, BX - 1)):
                part = pl.ds(base * BX + place, 8, stride=BX)
                layers[part, :] = layers[part, :] + xr[side, pl.ds(base, 8), :]
            lax.fori_loop(base, base + 8, outer, 0, unroll=4)

    def gx_copies(source, target, send, recv):
        for s in (1, 3, 2, 0):
            peer = (gx + s) % 4
            if s:
                remote(source(peer), target, sent.at[send], recv, gx=peer).start()
            else:
                here(source(gx), target, recv)

    def row_copies(source, target, send, recv):
        for offset in X_OFFSETS:
            a, low = row_peer(offset)
            remote(
                source(a, low), target, sent.at[send], recv, gy=a, gz=z_chip * 2 + low
            ).start()
        here(source(gy, x_low), target, recv)

    def first(k):
        gx_copies(
            lambda a: up.at[pl.ds(8 * k + 2 * a, 2)],
            xa.at[k, :, rows(gx * 128, 128), :],
            0,
            xa_sem.at[k],
        )
        row_copies(
            lambda a, low: up.at[32 + 8 * k + 2 * a + low],
            yb.at[k, x_low, :, lanes(gy)],
            1,
            yb_sem.at[k],
        )

    def second_a(k):
        row_copies(
            lambda a, low: xa.at[k, :, rows((2 * a + low) * 64, 64), :],
            ya.at[k, x_low, :, :, lanes(gy)],
            2,
            ya_sem.at[k],
        )

    def second_b(k):
        gx_copies(
            lambda a: yb.at[k, :, :, lanes(a)],
            xb.at[k, :, rows(gx * 128, 128), :],
            3,
            xb_sem.at[k],
        )

    def third_a(k, h_):
        def part(h):
            def source(y, z):
                return ya.at[k, :, :, rows(16 * z + 8 * h, 8), lanes(y)]

            target = zb.at[h, pl.ds(2 * z_chip, 2), pl.ds(8 * k + 2 * gx, 2)]

            def send(s, carry):
                y, z = side_peer(s)
                remote(
                    source(y, z), target, sent.at[4], zb_sem.at[h], gx=y, gz=z * 2 + x_low
                ).start()
                return carry

            lax.fori_loop(1, 16, send, 0)
            here(source(gx, z_chip), target, zb_sem.at[h])

        part(h_)

    def third_b(k, h_):
        def part(h):
            def source(a, b):
                return xb.at[k, :, rows((2 * a + b % 2) * 64 + 16 * (b // 2) + 8 * h, 8), :]

            target = zb.at[h, pl.ds(2 * z_chip, 2), 32 + 8 * k + mine]

            def send(s, carry):
                a, b = plane_peer(s)
                remote(source(a, b), target, sent.at[5], zb_sem.at[h], gy=a, gz=b).start()
                return carry

            lax.fori_loop(1, 32, send, 0)
            here(source(gy, gz), target, zb_sem.at[h])

        part(h_)

    def back_third(k, h):
        def source_a(y, z):
            return zb.at[h, pl.ds(2 * z, 2), pl.ds(8 * k + 2 * y, 2)]

        target_a = ya2.at[k, :, :, rows(16 * z_chip + 8 * h, 8), lanes(gx)]

        def send_a(s, carry):
            y, z = side_peer(s)
            remote(
                source_a(y, z), target_a, sent.at[6], ya2_sem.at[k], gx=y, gz=z * 2 + x_low
            ).start()
            return carry

        def source_b(a, b):
            return zb.at[h, pl.ds(2 * (b // 2), 2), 32 + 8 * k + 2 * a + b % 2]

        target_b = xb2.at[k, :, rows(mine * 64 + 16 * z_chip + 8 * h, 8), :]

        def send_b(s, carry):
            a, b = plane_peer(s)
            remote(source_b(a, b), target_b, sent.at[7], xb2_sem.at[k], gy=a, gz=b).start()
            return carry

        lax.fori_loop(1, 16, send_a, 0)
        here(source_a(gx, z_chip), target_a, ya2_sem.at[k])
        lax.fori_loop(1, 32, send_b, 0)
        here(source_b(gy, gz), target_b, xb2_sem.at[k])

    def back_second_a(k):
        row_copies(
            lambda a, low: ya2.at[k, low, :, :, lanes(a)],
            xa2.at[k, :, rows(mine * 64, 64), :],
            8,
            xa2_sem.at[k],
        )

    def back_second_b(k):
        gx_copies(
            lambda a: xb2.at[k, :, rows(a * 128, 128), :],
            yb2.at[k, :, :, lanes(gx)],
            9,
            yb2_sem.at[k],
        )

    def back_first_a(k):
        gx_copies(
            lambda a: xa2.at[k, :, rows(a * 128, 128), :],
            o_ref.at[pl.ds(8 * k + 2 * gx, 2)],
            10,
            out_sem,
        )

    def back_first_b(k):
        row_copies(
            lambda a, low: yb2.at[k, low, :, lanes(a)],
            o_ref.at[32 + 8 * k + mine],
            11,
            out_sem,
        )

    def x_pass(ref, inverse):
        low = jnp.concatenate([ref[0, :HALF], ref[1, :HALF]], axis=1)
        high = jnp.concatenate([ref[0, HALF:], ref[1, HALF:]], axis=1)
        if inverse:
            even = matmul(left[0], thirds(low, 0))
            odd = matmul(left[2], thirds(high, 0))
            low, high = even + odd, even - odd
        else:
            plus, minus = thirds(low + high, 0), thirds(low - high, 0)
            low, high = matmul(left[0], plus), matmul(left[1], minus)
        ref[0, :HALF], ref[1, :HALF] = low[:, :BY], low[:, BY:]
        ref[0, HALF:], ref[1, HALF:] = high[:, :BY], high[:, BY:]

    def y_pass(ref, inverse):
        flat = ref.reshape(256, N)

        def block(i, carry):
            part = rows(i * 128, 128)
            low, high = flat[part, :HALF], flat[part, HALF:]
            if inverse:
                even = matmul(thirds(low, 1), right[0])
                odd = matmul(thirds(high, 1), right[2])
                low, high = even + odd, even - odd
            else:
                plus, minus = thirds(low + high, 1), thirds(low - high, 1)
                low, high = matmul(plus, right[0]), matmul(minus, right[1])
            flat[part, :HALF] = low
            flat[part, HALF:] = high
            return carry

        lax.fori_loop(0, 2, block, 0)

    def start(k):
        outer_chunk(k)
        first(k)

    def second(k):
        drain(yb.at[k], yb_sem.at[k])
        y_pass(yb.at[k], False)
        second_b(k)
        drain(xa.at[k], xa_sem.at[k])
        x_pass(xa.at[k], False)
        second_a(k)

    def meet(k):
        for other in columns:
            pl.semaphore_signal(ready, inc=1, device_id={"gz": other}, device_id_type=MESH)
        pl.semaphore_wait(ready, 3)

    def third(k):
        drain(xb.at[k], xb_sem.at[k])
        x_pass(xb.at[k], False)
        third_b(k, 0)
        drain(ya.at[k], ya_sem.at[k])
        y_pass(ya.at[k], False)
        third_a(k, 0)
        third_b(k, 1)
        third_a(k, 1)

    def gather(k):
        for s in (1, 2, 3):
            remote(ms.at[0], ms.at[s], m_send.at[0], m_recv.at[0], gx=(gx + s) % 4).start()

    def spread(s, carry):
        a, b = plane_peer(s)
        remote(mb.at[0], mb.at[s], m_send.at[1], m_recv.at[1], gy=a, gz=b).start()
        return carry

    def share(k):
        drain(ms.at[pl.ds(1, 3)], m_recv.at[0])
        mb[0] = ms[0] + ms[1] + ms[2] + ms[3]
        lax.fori_loop(1, 32, spread, 0)

    def fill(k, carry):
        part = rows(k * 32, 32)
        waves[part, :] = wave_of(iota((32, BY), 0) + k * 32) + wave_of(iota((32, BY), 1) + gx * BY)
        return carry

    def prepare(k):
        lax.fori_loop(0, N // 32, fill, 0)
        for copy in loads:
            copy.wait()

    steps = dict(F=start, I=inner_chunk, S=second, T=third, M=meet, G=gather, H=share, P=prepare)
    for name, k in FORWARD:
        steps[name](k)

    drain(mb.at[pl.ds(1, 31)], m_recv.at[1])
    mobility = jnp.sum(jnp.sum(mb[...], axis=0), keepdims=True)
    factor = (step_length * stiffness) * (mobility / float(N * N * N))

    def z_stage(h):
        drain(zb.at[h], zb_sem.at[h])
        field = zb.at[h].reshape(N * 8, BY)

        def pair(i, carry):
            x0, x1 = 2 * i, 2 * i + 1

            def take(base):
                return jnp.concatenate(
                    [
                        field[pl.ds(base * 8 + x0, HALF, stride=8), :],
                        field[pl.ds(base * 8 + x1, HALF, stride=8), :],
                    ],
                    axis=1,
                )

            position = mine * 64 + 16 * z_chip + 8 * h
            wave0, wave1 = wave_of(position + x0), wave_of(position + x1)
            low, high = take(0), take(HALF)
            parts = []
            for value, table, back, base in (
                (low + high, 0, 0, 0),
                (low - high, 1, 2, HALF),
            ):
                value = matmul(left[table], thirds(value, 0))
                wave = waves[pl.ds(base, HALF), :]
                wave = jnp.concatenate([wave + wave0, wave + wave1], axis=1)
                value = value / (1.0 + factor * (wave * wave))
                parts.append(matmul(left[back], thirds(value, 0)))
            for base, value in ((0, parts[0] + parts[1]), (HALF, parts[0] - parts[1])):
                field[pl.ds(base * 8 + x0, HALF, stride=8), :] = value[:, :BY]
                field[pl.ds(base * 8 + x1, HALF, stride=8), :] = value[:, BY:]
            return carry

        lax.fori_loop(0, 4, pair, 0)
        back_third(0, h)

    def back_both(k):
        back_third(k, 0)
        back_third(k, 1)

    def inverse_two(k):
        drain(ya2.at[k], ya2_sem.at[k])
        y_pass(ya2.at[k], True)
        back_second_a(k)
        drain(xb2.at[k], xb2_sem.at[k])
        x_pass(xb2.at[k], True)
        back_second_b(k)

    def inverse_one(k):
        drain(xa2.at[k], xa2_sem.at[k])
        x_pass(xa2.at[k], True)
        back_first_a(k)
        drain(yb2.at[k], yb2_sem.at[k])
        y_pass(yb2.at[k], True)
        back_first_b(k)

    steps = dict(Z=z_stage, T=back_both, S=inverse_two, F=inverse_one)
    for name, k in BACKWARD:
        steps[name](k)
    drain(o_ref, out_sem)

    for i, count in enumerate((24, 28, 28, 24, 30, 31, 30, 31, 28, 24, 24, 28)):
        drain(up.at[pl.ds(0, count)], sent.at[i])
    drain(ms.at[pl.ds(1, 3)], m_send.at[0])
    drain(mb.at[pl.ds(1, 31)], m_send.at[1])


def local(concentration):
    left, right = tables()
    vmem, dma = pltpu.VMEM, pltpu.SemaphoreType.DMA
    any_space = pl.BlockSpec(memory_space=pl.ANY)
    hbm = pl.BlockSpec(memory_space=pltpu.HBM)
    x_field = vmem((CHUNKS, 2, N, BY), F32)
    ya_field = vmem((CHUNKS, 2, 2, 64, N), F32)
    yb_field = vmem((CHUNKS, 2, BX, N), F32)
    return pl.pallas_call(
        kernel,
        out_shape=jax.ShapeDtypeStruct((BZ, BX, BY), F32),
        in_specs=[hbm] * 3,
        out_specs=any_space,
        scratch_shapes=[
            vmem((BZ, BX, BY), F32),
            vmem((2, BZ, BY), F32),
            vmem((2, BZ, BY), F32),
            vmem((BX, BY), F32),
            vmem((2, BX, BY), F32),
            vmem((BX, BY), F32),
            vmem((2, BX, BY), F32),
            vmem((BZ, BX, BY), F32),
            x_field,
            ya_field,
            yb_field,
            x_field,
            vmem((2, 8, BZ, 8, BY), F32),
            ya_field,
            x_field,
            x_field,
            yb_field,
            vmem((N, BY), F32),
            vmem((3, HALF, 3 * HALF), BF16),
            vmem((3, 3 * HALF, HALF), BF16),
            vmem((4, 8, BY), F32),
            vmem((32, 8, BY), F32),
            dma,
            dma((4,)),
            dma((6,)),
            dma((6,)),
            dma((12,)),
            dma((CHUNKS,)),
            dma((CHUNKS,)),
            dma((CHUNKS,)),
            dma((CHUNKS,)),
            dma((2,)),
            dma((CHUNKS,)),
            dma((CHUNKS,)),
            dma((CHUNKS,)),
            dma((CHUNKS,)),
            dma,
            dma((2,)),
            dma((2,)),
            pltpu.SemaphoreType.REGULAR,
        ],
        compiler_params=pltpu.CompilerParams(
            collective_id=0, has_side_effects=True, vmem_limit_bytes=44 * 2**20
        ),
    )(concentration, jnp.asarray(left), jnp.asarray(right))


def solution(mesh):
    spec = P("gz", "gx", "gy")
    return jax.shard_map(local, mesh=mesh, in_specs=(spec,), out_specs=spec, check_vma=False)
```

```python
import functools

import jax
import jax.numpy as jnp
import numpy as np
from jax import lax
from jax.experimental import pallas as pl
from jax.experimental.pallas import tpu as pltpu
from jax.sharding import PartitionSpec as P

MESH = pl.DeviceIdType.MESH
F32, BF16 = jnp.float32, jnp.bfloat16

step_length = 0.2
stiffness = 0.25

N = 512
HALF = N // 2
BZ, BX, BY = 64, 128, 128
CHUNKS = 4
FORWARD = (
    ("F", 0), ("F", 1), ("I", 2), ("I", 3), ("G", 0), ("P", 0), ("S", 0), ("F", 2), ("S", 1),
    ("M", 0), ("H", 0), ("F", 3), ("T", 0), ("S", 2), ("T", 1), ("S", 3), ("T", 2), ("T", 3),
)
BACKWARD = (
    ("Z", 0), ("U", 0), ("Z", 1), ("U", 1), ("S", 0), ("T", 2), ("S", 1), ("T", 3), ("F", 0), ("S", 2),
    ("F", 1), ("S", 3), ("F", 2), ("F", 3),
)
X_OFFSETS = ((1, 0), (3, 0), (2, 0), (1, 1), (3, 1), (2, 1), (0, 1))


def split_table(matrix):
    high = matrix.astype(np.float32).astype(jnp.bfloat16)
    low = (matrix - high.astype(np.float64)).astype(np.float32).astype(jnp.bfloat16)
    return high, low


def tables():
    index = np.arange(N)
    angle = 2.0 * np.pi / N * (index[:, None] * index[None, :] % N)
    hartley = (np.cos(angle) + np.sin(angle)) / np.sqrt(N)
    even, odd = hartley[0::2, :HALF], hartley[1::2, :HALF]
    left, right = [], []
    for matrix in (even, odd, odd.T):
        high, low = split_table(matrix)
        left.append(np.concatenate([high, low], axis=1))
    for matrix in (even, odd.T, odd):
        high, low = split_table(matrix)
        right.append(np.concatenate([high, low], axis=0))
    return np.stack(left), np.stack(right)


def thirds(a, axis):
    high = a.astype(BF16)
    low = (a - high.astype(F32)).astype(BF16)
    return jnp.concatenate([high, high, low], axis=axis)


def matmul(a, b):
    return jnp.dot(a, b, preferred_element_type=F32)


def wave_of(position):
    true = jnp.where(position < HALF, 2 * position, 2 * position - (N - 1))
    folded = jnp.minimum(true, N - true).astype(F32)
    wave = (2.0 * np.pi / N) * folded
    return wave * wave


def iota(shape, dim):
    return lax.broadcasted_iota(jnp.int32, shape, dim)


def kernel(
    c_ref,
    left_hbm,
    right_hbm,
    o_ref,
    cz,
    xs,
    xr,
    ye,
    yr,
    yc,
    zr,
    up,
    xa,
    ya,
    yb,
    xb,
    zb,
    ya2,
    xb2,
    xa2,
    yb2,
    waves,
    left,
    right,
    ms,
    mb,
    local_sem,
    table_sem,
    halo_send,
    halo_recv,
    sent,
    xa_sem,
    ya_sem,
    yb_sem,
    xb_sem,
    zb_sem,
    ya2_sem,
    xb2_sem,
    xa2_sem,
    yb2_sem,
    out_sem,
    m_send,
    m_recv,
    ready,
):
    gx, gy, gz = lax.axis_index("gx"), lax.axis_index("gy"), lax.axis_index("gz")
    z_chip, x_low = gz // 2, gz % 2
    x_chip, core = (gy // 2) * 2 + x_low, gy % 2
    mine = gy * 2 + x_low

    def plane_peer(s):
        k = s % 16
        dx = k % 4
        dz = (k // 4 + dx) % 4
        px, pz, pc = (x_chip + dx) % 4, (z_chip + dz) % 4, (core + s // 16) % 2
        return (px // 2) * 2 + pc, pz * 2 + px % 2

    def row_peer(offset):
        px, pc = (x_chip + offset[0]) % 4, (core + offset[1]) % 2
        return (px // 2) * 2 + pc, px % 2

    def side_peer(s):
        dy = s % 4
        return (gx + dy) % 4, (z_chip + s // 4 + dy) % 4

    def remote(src, dst, send, recv, **where):
        return pltpu.make_async_remote_copy(
            src, dst, send, recv, device_id=where, device_id_type=MESH
        )

    def here(src, dst, recv):
        pltpu.make_async_copy(src, dst, recv).start()

    def drain(ref, sem):
        pltpu.make_async_copy(ref, ref, sem).wait()

    def lanes(block):
        return pl.ds(pl.multiple_of(block * 128, 128), 128)

    def rows(start, size):
        return pl.ds(pl.multiple_of(start, size), size)

    load = pltpu.make_async_copy(c_ref, cz, local_sem)
    load.start()
    pair, third = pl.ds(0, N), pl.ds(N, HALF)
    loads = [
        pltpu.make_async_copy(left_hbm, left.at[:, :, pair], table_sem.at[0]),
        pltpu.make_async_copy(left_hbm.at[:, :, pl.ds(0, HALF)], left.at[:, :, third], table_sem.at[1]),
        pltpu.make_async_copy(right_hbm, right.at[:, pair], table_sem.at[2]),
        pltpu.make_async_copy(right_hbm.at[:, pl.ds(0, HALF)], right.at[:, third], table_sem.at[3]),
    ]
    for copy in loads:
        copy.start()
    barrier = pltpu.get_barrier_semaphore()

    for offset in X_OFFSETS:
        a, low = row_peer(offset)
        pl.semaphore_signal(
            barrier, inc=1, device_id={"gy": a, "gz": z_chip * 2 + low}, device_id_type=MESH
        )
    across = ((z_chip + 3 - 2 * x_low) % 4) * 2 + 1 - x_low
    columns = [((z_chip + s) % 4) * 2 + x_low for s in (1, 2, 3)]
    for s in (1, 2, 3):
        pl.semaphore_signal(
            barrier, inc=1, device_id={"gx": (gx + s) % 4}, device_id_type=MESH
        )
    for other in columns + [across]:
        pl.semaphore_signal(barrier, inc=1, device_id={"gz": other}, device_id_type=MESH)
    load.wait()

    flat = cz.reshape(BZ * BX, BY)
    xs[0] = flat[pl.ds(0, BZ, stride=BX), :]
    xs[1] = flat[pl.ds(BX - 1, BZ, stride=BX), :]
    lane = iota((BX, BY), 1)
    row = iota((BX, BY), 0)

    def pack(z, acc):
        turned = pltpu.roll(cz[z], 2 * z, 1)
        keep = (lane == 2 * z) | (lane == (2 * z + BY - 1) % BY)
        return jnp.where(keep, turned, acc)

    ye[...] = lax.fori_loop(0, BZ, pack, jnp.zeros((BX, BY), F32), unroll=4)

    def terms(c):
        square = c * c
        return square * c - c, 1.05 - square

    def inner(z, total):
        c = cz[z]
        p, m = terms(c)
        pz, mz = terms(cz[jnp.minimum(z + 1, BZ - 1)])
        divergence = (m + mz) * (pz - p)
        pz, mz = terms(cz[jnp.maximum(z - 1, 0)])
        divergence = divergence - (m + mz) * (p - pz)
        before = jnp.where(row == 0, p, pltpu.roll(p, 1, 0))
        flux = (m + pltpu.roll(m, 1, 0)) * (p - before)
        divergence = divergence + (pltpu.roll(flux, BX - 1, 0) - flux)
        before = jnp.where(lane == 0, p, pltpu.roll(p, 1, 1))
        flux = (m + pltpu.roll(m, 1, 1)) * (p - before)
        divergence = divergence + (pltpu.roll(flux, BY - 1, 1) - flux)
        up[z] = c + (0.5 * step_length) * divergence
        return total + jnp.sum(m.reshape(16, 8, BY), axis=0)

    def inner_chunk(k):
        total = lax.fori_loop(8 * k, 8 * k + 8, inner, jnp.zeros((8, BY), F32), unroll=2)
        total = lax.fori_loop(32 + 8 * k, 40 + 8 * k, inner, total, unroll=2)
        ms[0] = total if k == 0 else ms[0] + total

    pl.semaphore_wait(barrier, 14)
    halo = [
        remote(ye, yr.at[0], halo_send.at[4], halo_recv.at[4], gy=(gy + 1) % 4),
        remote(ye, yr.at[1], halo_send.at[5], halo_recv.at[5], gy=(gy + 3) % 4),
        remote(c_ref.at[BZ - 1], zr.at[0], halo_send.at[0], halo_recv.at[0], gz=(gz + 1) % 8),
        remote(c_ref.at[0], zr.at[1], halo_send.at[1], halo_recv.at[1], gz=(gz + 7) % 8),
        remote(xs.at[1], xr.at[0], halo_send.at[2], halo_recv.at[2], gx=(gx + 1) % 4),
        remote(xs.at[0], xr.at[1], halo_send.at[3], halo_recv.at[3], gx=(gx + 3) % 4),
    ]
    for copy in halo:
        copy.start()
    inner_chunk(0)
    inner_chunk(1)
    for copy in halo:
        copy.wait()

    def inflow(inside, outside):
        p, m = terms(inside)
        ph, mh = terms(outside)
        return (0.5 * step_length) * ((m + mh) * (ph - p))

    yc[...] = inflow(
        ye[...], jnp.where(lane % 2 == 0, pltpu.roll(yr[0], 1, 1), pltpu.roll(yr[1], BY - 1, 1))
    )
    xr[0] = inflow(xs[0], xr[0])
    xr[1] = inflow(xs[1], xr[1])
    edge = (lane == 0) | (lane == BY - 1)
    layers = up.reshape(BZ * BX, BY)

    def outer(z, carry):
        turned = pltpu.roll(yc[...], (BY - 2 * z) % BY, 1)
        up[z] = up[z] + jnp.where(edge, turned, 0.0)
        return carry

    def outer_chunk(k):
        if k == 0:
            up[0] = up[0] + inflow(cz[0], zr[0])
        if k == CHUNKS - 1:
            up[BZ - 1] = up[BZ - 1] + inflow(cz[BZ - 1], zr[1])
        for base in (8 * k, 32 + 8 * k):
            for side, place in ((0, 0), (1, BX - 1)):
                part = pl.ds(base * BX + place, 8, stride=BX)
                layers[part, :] = layers[part, :] + xr[side, pl.ds(base, 8), :]
            lax.fori_loop(base, base + 8, outer, 0, unroll=4)

    def gx_copies(source, target, send, recv):
        for s in (1, 3, 2, 0):
            peer = (gx + s) % 4
            if s:
                remote(source(peer), target, sent.at[send], recv, gx=peer).start()
            else:
                here(source(gx), target, recv)

    def row_copies(source, target, send, recv):
        for offset in X_OFFSETS:
            a, low = row_peer(offset)
            remote(
                source(a, low), target, sent.at[send], recv, gy=a, gz=z_chip * 2 + low
            ).start()
        here(source(gy, x_low), target, recv)

    def first(k):
        gx_copies(
            lambda a: up.at[pl.ds(8 * k + 2 * a, 2)],
            xa.at[k, :, rows(gx * 128, 128), :],
            0,
            xa_sem.at[k],
        )
        row_copies(
            lambda a, low: up.at[32 + 8 * k + 2 * a + low],
            yb.at[k, x_low, :, lanes(gy)],
            1,
            yb_sem.at[k],
        )

    def second_a(k):
        row_copies(
            lambda a, low: xa.at[k, :, rows((2 * a + low) * 64, 64), :],
            ya.at[k, x_low, :, :, lanes(gy)],
            2,
            ya_sem.at[k],
        )

    def second_b(k):
        gx_copies(
            lambda a: yb.at[k, :, :, lanes(a)],
            xb.at[k, :, rows(gx * 128, 128), :],
            3,
            xb_sem.at[k],
        )

    def third_a(k, h_):
        def part(h):
            def source(y, z):
                return ya.at[k, :, :, rows(16 * z + 8 * h, 8), lanes(y)]

            target = zb.at[h, pl.ds(2 * z_chip, 2), pl.ds(8 * k + 2 * gx, 2)]

            def send(s, carry):
                y, z = side_peer(s)
                remote(
                    source(y, z), target, sent.at[4], zb_sem.at[h], gx=y, gz=z * 2 + x_low
                ).start()
                return carry

            lax.fori_loop(1, 16, send, 0)
            here(source(gx, z_chip), target, zb_sem.at[h])

        part(h_)

    def third_b(k, h_):
        def part(h):
            def source(a, b):
                return xb.at[k, :, rows((2 * a + b % 2) * 64 + 16 * (b // 2) + 8 * h, 8), :]

            target = zb.at[h, pl.ds(2 * z_chip, 2), 32 + 8 * k + mine]

            def send(s, carry):
                a, b = plane_peer(s)
                remote(source(a, b), target, sent.at[5], zb_sem.at[h], gy=a, gz=b).start()
                return carry

            lax.fori_loop(1, 32, send, 0)
            here(source(gy, gz), target, zb_sem.at[h])

        part(h_)

    def back_third(k, h):
        def source_a(y, z):
            return zb.at[h, pl.ds(2 * z, 2), pl.ds(8 * k + 2 * y, 2)]

        target_a = ya2.at[k, :, :, rows(16 * z_chip + 8 * h, 8), lanes(gx)]

        def send_a(s, carry):
            y, z = side_peer(s)
            remote(
                source_a(y, z), target_a, sent.at[6], ya2_sem.at[k], gx=y, gz=z * 2 + x_low
            ).start()
            return carry

        def source_b(a, b):
            return zb.at[h, pl.ds(2 * (b // 2), 2), 32 + 8 * k + 2 * a + b % 2]

        target_b = xb2.at[k, :, rows(mine * 64 + 16 * z_chip + 8 * h, 8), :]

        def send_b(s, carry):
            a, b = plane_peer(s)
            remote(source_b(a, b), target_b, sent.at[7], xb2_sem.at[k], gy=a, gz=b).start()
            return carry

        lax.fori_loop(1, 16, send_a, 0)
        here(source_a(gx, z_chip), target_a, ya2_sem.at[k])
        lax.fori_loop(1, 32, send_b, 0)
        here(source_b(gy, gz), target_b, xb2_sem.at[k])

    def back_second_a(k):
        row_copies(
            lambda a, low: ya2.at[k, low, :, :, lanes(a)],
            xa2.at[k, :, rows(mine * 64, 64), :],
            8,
            xa2_sem.at[k],
        )

    def back_second_b(k):
        gx_copies(
            lambda a: xb2.at[k, :, rows(a * 128, 128), :],
            yb2.at[k, :, :, lanes(gx)],
            9,
            yb2_sem.at[k],
        )

    def back_first_a(k):
        gx_copies(
            lambda a: xa2.at[k, :, rows(a * 128, 128), :],
            o_ref.at[pl.ds(8 * k + 2 * gx, 2)],
            10,
            out_sem,
        )

    def back_first_b(k):
        row_copies(
            lambda a, low: yb2.at[k, low, :, lanes(a)],
            o_ref.at[32 + 8 * k + mine],
            11,
            out_sem,
        )

    def x_pass(ref, inverse):
        low = jnp.concatenate([ref[0, :HALF], ref[1, :HALF]], axis=1)
        high = jnp.concatenate([ref[0, HALF:], ref[1, HALF:]], axis=1)
        if inverse:
            even = matmul(left[0], thirds(low, 0))
            odd = matmul(left[2], thirds(high, 0))
            low, high = even + odd, even - odd
        else:
            plus, minus = thirds(low + high, 0), thirds(low - high, 0)
            low, high = matmul(left[0], plus), matmul(left[1], minus)
        ref[0, :HALF], ref[1, :HALF] = low[:, :BY], low[:, BY:]
        ref[0, HALF:], ref[1, HALF:] = high[:, :BY], high[:, BY:]

    def y_pass(ref, inverse):
        flat = ref.reshape(256, N)

        def block(i, carry):
            part = rows(i * 128, 128)
            low, high = flat[part, :HALF], flat[part, HALF:]
            if inverse:
                even = matmul(thirds(low, 1), right[0])
                odd = matmul(thirds(high, 1), right[2])
                low, high = even + odd, even - odd
            else:
                plus, minus = thirds(low + high, 1), thirds(low - high, 1)
                low, high = matmul(plus, right[0]), matmul(minus, right[1])
            flat[part, :HALF] = low
            flat[part, HALF:] = high
            return carry

        lax.fori_loop(0, 2, block, 0)

    def start(k):
        outer_chunk(k)
        first(k)

    def second(k):
        drain(yb.at[k], yb_sem.at[k])
        y_pass(yb.at[k], False)
        second_b(k)
        drain(xa.at[k], xa_sem.at[k])
        x_pass(xa.at[k], False)
        second_a(k)

    def meet(k):
        for other in columns:
            pl.semaphore_signal(ready, inc=1, device_id={"gz": other}, device_id_type=MESH)
        pl.semaphore_wait(ready, 3)

    def third(k):
        drain(xb.at[k], xb_sem.at[k])
        x_pass(xb.at[k], False)
        third_b(k, 0)
        drain(ya.at[k], ya_sem.at[k])
        y_pass(ya.at[k], False)
        third_a(k, 0)
        third_b(k, 1)
        third_a(k, 1)

    def gather(k):
        for s in (1, 2, 3):
            remote(ms.at[0], ms.at[s], m_send.at[0], m_recv.at[0], gx=(gx + s) % 4).start()

    def spread(s, carry):
        a, b = plane_peer(s)
        remote(mb.at[0], mb.at[s], m_send.at[1], m_recv.at[1], gy=a, gz=b).start()
        return carry

    def share(k):
        drain(ms.at[pl.ds(1, 3)], m_recv.at[0])
        mb[0] = ms[0] + ms[1] + ms[2] + ms[3]
        lax.fori_loop(1, 32, spread, 0)

    def fill(k, carry):
        part = rows(k * 32, 32)
        waves[part, :] = wave_of(iota((32, BY), 0) + k * 32) + wave_of(iota((32, BY), 1) + gx * BY)
        return carry

    def prepare(k):
        lax.fori_loop(0, N // 32, fill, 0)
        for copy in loads:
            copy.wait()

    steps = dict(F=start, I=inner_chunk, S=second, T=third, M=meet, G=gather, H=share, P=prepare)
    for name, k in FORWARD:
        steps[name](k)

    drain(mb.at[pl.ds(1, 31)], m_recv.at[1])
    mobility = jnp.sum(jnp.sum(mb[...], axis=0), keepdims=True)
    factor = (step_length * stiffness) * (mobility / float(N * N * N))

    def z_stage(h):
        drain(zb.at[h], zb_sem.at[h])
        field = zb.at[h].reshape(N * 8, BY)

        def pair(i, carry):
            x0, x1 = 2 * i, 2 * i + 1

            def take(base):
                return jnp.concatenate(
                    [
                        field[pl.ds(base * 8 + x0, HALF, stride=8), :],
                        field[pl.ds(base * 8 + x1, HALF, stride=8), :],
                    ],
                    axis=1,
                )

            position = mine * 64 + 16 * z_chip + 8 * h
            wave0, wave1 = wave_of(position + x0), wave_of(position + x1)
            low, high = take(0), take(HALF)
            parts = []
            for value, table, back, base in (
                (low + high, 0, 0, 0),
                (low - high, 1, 2, HALF),
            ):
                value = matmul(left[table], thirds(value, 0))
                wave = waves[pl.ds(base, HALF), :]
                wave = jnp.concatenate([wave + wave0, wave + wave1], axis=1)
                value = value / (1.0 + factor * (wave * wave))
                parts.append(matmul(left[back], thirds(value, 0)))
            for base, value in ((0, parts[0] + parts[1]), (HALF, parts[0] - parts[1])):
                field[pl.ds(base * 8 + x0, HALF, stride=8), :] = value[:, :BY]
                field[pl.ds(base * 8 + x1, HALF, stride=8), :] = value[:, BY:]
            return carry

        lax.fori_loop(0, 4, pair, 0)
        back_third(0, h)

    def back_both(k):
        back_third(k, 0)
        back_third(k, 1)

    def inverse_two(k):
        drain(ya2.at[k], ya2_sem.at[k])
        y_pass(ya2.at[k], True)
        back_second_a(k)
        drain(xb2.at[k], xb2_sem.at[k])
        x_pass(xb2.at[k], True)
        back_second_b(k)

    def inverse_one(k):
        drain(xa2.at[k], xa2_sem.at[k])
        x_pass(xa2.at[k], True)
        back_first_a(k)
        drain(yb2.at[k], yb2_sem.at[k])
        y_pass(yb2.at[k], True)
        back_first_b(k)

    def early(h):
        back_third(1, h)

    steps = dict(U=early, Z=z_stage, T=back_both, S=inverse_two, F=inverse_one)
    for name, k in BACKWARD:
        steps[name](k)
    drain(o_ref, out_sem)

    for i, count in enumerate((24, 28, 28, 24, 30, 31, 30, 31, 28, 24, 24, 28)):
        drain(up.at[pl.ds(0, count)], sent.at[i])
    drain(ms.at[pl.ds(1, 3)], m_send.at[0])
    drain(mb.at[pl.ds(1, 31)], m_send.at[1])


def local(concentration):
    left, right = tables()
    vmem, dma = pltpu.VMEM, pltpu.SemaphoreType.DMA
    any_space = pl.BlockSpec(memory_space=pl.ANY)
    hbm = pl.BlockSpec(memory_space=pltpu.HBM)
    x_field = vmem((CHUNKS, 2, N, BY), F32)
    ya_field = vmem((CHUNKS, 2, 2, 64, N), F32)
    yb_field = vmem((CHUNKS, 2, BX, N), F32)
    return pl.pallas_call(
        kernel,
        out_shape=jax.ShapeDtypeStruct((BZ, BX, BY), F32),
        in_specs=[hbm] * 3,
        out_specs=any_space,
        scratch_shapes=[
            vmem((BZ, BX, BY), F32),
            vmem((2, BZ, BY), F32),
            vmem((2, BZ, BY), F32),
            vmem((BX, BY), F32),
            vmem((2, BX, BY), F32),
            vmem((BX, BY), F32),
            vmem((2, BX, BY), F32),
            vmem((BZ, BX, BY), F32),
            x_field,
            ya_field,
            yb_field,
            x_field,
            vmem((2, 8, BZ, 8, BY), F32),
            ya_field,
            x_field,
            x_field,
            yb_field,
            vmem((N, BY), F32),
            vmem((3, HALF, 3 * HALF), BF16),
            vmem((3, 3 * HALF, HALF), BF16),
            vmem((4, 8, BY), F32),
            vmem((32, 8, BY), F32),
            dma,
            dma((4,)),
            dma((6,)),
            dma((6,)),
            dma((12,)),
            dma((CHUNKS,)),
            dma((CHUNKS,)),
            dma((CHUNKS,)),
            dma((CHUNKS,)),
            dma((2,)),
            dma((CHUNKS,)),
            dma((CHUNKS,)),
            dma((CHUNKS,)),
            dma((CHUNKS,)),
            dma,
            dma((2,)),
            dma((2,)),
            pltpu.SemaphoreType.REGULAR,
        ],
        compiler_params=pltpu.CompilerParams(
            collective_id=0, has_side_effects=True, vmem_limit_bytes=44 * 2**20
        ),
    )(concentration, jnp.asarray(left), jnp.asarray(right))


def solution(mesh):
    spec = P("gz", "gx", "gy")
    return jax.shard_map(local, mesh=mesh, in_specs=(spec,), out_specs=spec, check_vma=False)
```
